32 devices in a mesh: row: 4 (over y, x), col: 8 (over z, core).
Axes of the slice: x: 2, y: 2, z: 4, core: 2. Of those that a mesh axis runs over, the one named last changes fastest.
Arguments:
- factors: float32 [1, 8192, 8192], P(None, 'row', 'col'), may hold values from -20 to 30, as said below
Outputs:
- refreshed: float32 [1, 8192, 8192], P(None, 'row', 'col')
The draws below stay inside these ranges and needn't reach their ends.
Inputs may be any that keep to these rules, and one draw needn't show every extreme that they name: `factors`: every factor is symmetric positive definite.
All inputs are finite; a program needn't handle non-finite values.
Results may differ from the reference program's by a relative error of at most 0.0003.
Values sent between devices are 32-bit elements; how exact they have to be, the bound alone decides.
A program may use at most 64 MiB of HBM per device.

```python
import jax
import jax.numpy as jnp
from jax import lax

N = 8192
P_SIZE = 512
STEPS = 2
FACTORS = 1
N_COL = 8


def draw_factors(key, part):
    base_key = jax.random.fold_in(key, 11)
    position = jnp.arange(N, dtype=jnp.float32)
    rising = 3.0 ** (0.5 * position / N)
    scale_low, scale_high = (0.25, 0.75)

    def one_factor(member):
        noise_key, level_key, scale_key, shared_key = jax.random.split(jax.random.fold_in(base_key, member), 4)
        jitter = jax.random.normal(noise_key, (N, N), jnp.float32)
        shared = 0.5 * jax.random.truncated_normal(shared_key, -2.0, 2.0, (N, 8), jnp.float32)
        symmetric = (jitter + jitter.T) * (0.5 / jnp.sqrt(2.0 * N))
        common_part = jnp.dot(shared, shared.T, precision=lax.Precision.HIGHEST)
        levels = jax.random.uniform(level_key, (N,), jnp.float32, 2.0, 4.0)
        scales = jnp.exp(jax.random.uniform(scale_key, (N,), jnp.float32, jnp.log(scale_low), jnp.log(scale_high))) * rising
        matrix_core = symmetric + common_part + jnp.diag(levels)
        return scales[:, None] * matrix_core * scales[None, :]
    return lax.map(one_factor, jnp.arange(FACTORS))


def setup_inputs(seed: int = 0) -> dict:
    arg_keys = jax.random.split(jax.random.key(seed), 2)
    factors = draw_factors(jax.random.fold_in(arg_keys[1], 71), 0)
    return dict(factors=factors)


damping_share = 0.03162277660168379

def reference(factors):
    col_block = N // N_COL
    panel_slab = P_SIZE // N_COL
    sequence = jnp.arange(N, dtype=jnp.int32).reshape(N // col_block, col_block // panel_slab, panel_slab)
    sequence = sequence.transpose(1, 0, 2).reshape(N)
    restore = jnp.zeros((N,), jnp.int32).at[sequence].set(jnp.arange(N, dtype=jnp.int32))
    results = []
    for member in range(FACTORS):
        matrix = factors[member]
        damping = damping_share * jnp.trace(matrix) / N
        matrix = matrix + damping * jnp.eye(N, dtype=matrix.dtype)
        matrix = matrix[sequence][:, sequence]
        for section_no in range(STEPS):
            begin_at = section_no * P_SIZE
            finish = begin_at + P_SIZE
            factor_kk = jnp.linalg.cholesky(matrix[begin_at:finish, begin_at:finish])
            inverse_kk = jax.scipy.linalg.solve_triangular(factor_kk, jnp.eye(P_SIZE, dtype=matrix.dtype), lower=True)
            panel_rows = jnp.dot(matrix[finish:, begin_at:finish], inverse_kk.T, precision=lax.Precision.HIGHEST)
            update = jnp.dot(panel_rows, panel_rows.T, precision=lax.Precision.HIGHEST)
            matrix = matrix.at[finish:, finish:].add(-update)
            matrix = matrix.at[begin_at:finish, begin_at:finish].set(factor_kk)
            matrix = matrix.at[finish:, begin_at:finish].set(panel_rows)
            matrix = matrix.at[begin_at:finish, finish:].set(0.0)
        results.append(matrix[restore][:, restore])
    return jnp.stack(results)
```

```python
import functools

import jax
import jax.numpy as jnp
from jax import lax
from jax.experimental import pallas as pl
from jax.experimental.pallas import tpu as pltpu
from jax.sharding import PartitionSpec as P

P_SIZE = 512
STEPS = 2
TILE = 128

damping_share = 0.03162277660168379
top_precision = lax.Precision.HIGHEST
three_pass = lax.Precision.HIGH


def dot(a, b, dims, precision=top_precision):
    return lax.dot_general(
        a, b, (dims, ((), ())), precision=precision, preferred_element_type=jnp.float32
    )


def factor_tile(tile):
    size = tile.shape[0]
    groups = size // 8
    lane = lax.broadcasted_iota(jnp.int32, (8, size), 1)
    sub = lax.broadcasted_iota(jnp.int32, (8, size), 0)
    left = [tile[8 * t : 8 * t + 8, :] for t in range(groups)]
    right = [jnp.where(lane == sub + 8 * t, 1.0, 0.0).astype(jnp.float32) for t in range(groups)]

    def lanes(x, at):
        return jnp.broadcast_to(x[:, at : at + 1], x.shape)

    def rows(x, at):
        return jnp.broadcast_to(x[at : at + 1, :], x.shape)

    for j in range(groups):
        cols = [lanes(left[j], 8 * j + q) for q in range(8)]
        row_l, row_r = left[j], right[j]
        scales, coef, fin_l, fin_r = [], [], [], []
        out_l, out_r = row_l, row_r
        for i in range(8):
            pivot = rows(cols[i], i)
            s = lax.rsqrt(pivot)
            s = s * (1.5 - 0.5 * pivot * s * s)
            scales.append(s)
            l = cols[i] * s
            done_l = rows(row_l, i) * s
            done_r = rows(row_r, i) * s
            fin_l.append(done_l)
            fin_r.append(done_r)
            out_l = jnp.where(sub == i, done_l, out_l)
            out_r = jnp.where(sub == i, done_r, out_r)
            row_l = row_l - l * done_l
            row_r = row_r - l * done_r
            cq = {}
            for q in range(i + 1, 8):
                cq[q] = rows(l, q)
                cols[q] = cols[q] - l * cq[q]
            coef.append(cq)
        left[j] = jnp.where(lane >= sub + 8 * j, out_l, 0.0)
        right[j] = out_r
        for t in range(j + 1, groups):
            c = [lanes(left[t], 8 * j + q) for q in range(8)]
            acc_l, acc_r = left[t], right[t]
            for i in range(8):
                l = c[i] * scales[i]
                for q in range(i + 1, 8):
                    c[q] = c[q] - l * coef[i][q]
                acc_l = acc_l - l * fin_l[i]
                acc_r = acc_r - l * fin_r[i]
            left[t], right[t] = acc_l, acc_r
    return jnp.concatenate(left, axis=0), jnp.concatenate(right, axis=0)


def place_kernel(first_b, last_b, bpr, slab, order, at_ref, g_ref, s_ref, low_ref):
    total = STEPS * P_SIZE
    width = STEPS * slab
    per_tile = TILE // slab
    z_count, r_count = g_ref.shape[1], g_ref.shape[2]
    row_id, z_id, core = at_ref[0], at_ref[1], at_ref[2]

    def piece(r, c):
        z = lax.rem(c // 2 - z_id + z_count, z_count)
        return lax.rem(c + core, 2), z, jnp.bitwise_xor(r, row_id)

    def place(cp, carry):
        r, base = cp // bpr, (cp % bpr) * width
        for m in range(P_SIZE // TILE):
            where = [piece(r, m * per_tile + c) for c in range(per_tile)]
            for k in range(STEPS):
                got = [g_ref[i, j, l, pl.ds(base + k * slab, slab), :] for i, j, l in where]
                for kk in range(STEPS):
                    parts = [x[:, kk * slab : (kk + 1) * slab] for x in got]
                    s_ref[
                        pl.ds(pl.multiple_of(k * P_SIZE + cp * slab, 8), slab),
                        kk * P_SIZE + m * TILE : kk * P_SIZE + (m + 1) * TILE,
                    ] = jnp.concatenate(parts, axis=1)
        return carry

    lax.fori_loop(0, r_count * bpr, place, 0)
    trace = jnp.zeros((8, width), jnp.float32)
    for i in range(2):
        for j in range(z_count):
            for l in range(r_count):
                trace = trace + g_ref[i, j, l, bpr * width : bpr * width + 8, :]
    damping = damping_share * trace[0:1, 0:1] / order
    on_diag = lax.broadcasted_iota(jnp.int32, (TILE, TILE), 0) == lax.broadcasted_iota(
        jnp.int32, (TILE, TILE), 1
    )
    low_ref[...] = jnp.zeros_like(low_ref)

    def damp(b, carry):
        here = pl.ds(pl.multiple_of(b * TILE, TILE), TILE)
        tile = s_ref[here, here]
        s_ref[here, here] = tile + jnp.where(on_diag, jnp.broadcast_to(damping, tile.shape), 0.0)
        return carry

    lax.fori_loop(0, total // TILE, damp, 0)
    eliminate(first_b, last_b, s_ref, low_ref)


def eliminate(first_b, last_b, s_ref, low_ref):
    blocks = s_ref.shape[0] // TILE

    def step(b, carry):
        here = pl.ds(pl.multiple_of(b * TILE, TILE), TILE)
        upper, inverse = factor_tile(s_ref[here, here])
        low_ref[here, here] = upper.T
        s_ref[here, :] = dot(inverse, s_ref[here, :], ((1,), (0,)))
        s_ref[here, here] = inverse

        def trail(i, carry2):
            there = pl.ds(pl.multiple_of(i * TILE, TILE), TILE)
            low = dot(s_ref[there, here], inverse, ((1,), (1,)))
            low_ref[there, here] = low
            s_ref[there, here] = jnp.zeros((TILE, TILE), jnp.float32)
            s_ref[there, :] = s_ref[there, :] - dot(low, s_ref[here, :], ((1,), (0,)))
            return carry2

        lax.fori_loop(b + 1, blocks, trail, 0)
        return carry

    lax.fori_loop(first_b, last_b, step, 0)


def finish_kernel(
    first_b, last_b, bpr, slab, col_count, at_ref, s_in, low_in, inv_ref, own_ref, s_ref, low_ref
):
    total = STEPS * P_SIZE
    s_ref[...] = s_in[...]
    low_ref[...] = low_in[...]
    eliminate(first_b, last_b, s_ref, low_ref)

    def emit(i, carry):
        here = pl.ds(pl.multiple_of(i * TILE, TILE), TILE)
        value = s_ref[here, :]
        col = lax.broadcasted_iota(jnp.int32, value.shape, 1)
        value = jnp.where(col < (i + 1) * TILE, value, 0.0)
        for c in range(col_count):
            parts = [value[:, k * P_SIZE + c * slab :][:, :slab] for k in range(STEPS)]
            inv_ref[c, here, :] = jnp.concatenate(parts, axis=1)
        return carry

    lax.fori_loop(0, total // TILE, emit, 0)
    row_id = at_ref[0]
    col_id = at_ref[1] * 2 + at_ref[2]
    for c in range(col_count):

        @pl.when(col_id == c)
        def _():
            for b in range(bpr):
                for k in range(STEPS):
                    at = pl.multiple_of(k * P_SIZE + (row_id * bpr + b) * slab, 8)
                    value = low_ref[pl.ds(at, slab), :]
                    parts = [value[:, q * P_SIZE + c * slab :][:, :slab] for q in range(STEPS)]
                    own_ref[b, k * slab : (k + 1) * slab, :] = jnp.concatenate(parts, axis=1)


def in_vmem(count):
    return [pl.BlockSpec(memory_space=pltpu.VMEM)] * count


in_smem = pl.BlockSpec(memory_space=pltpu.SMEM)


def cost(flops):
    return pl.CostEstimate(flops=flops, bytes_accessed=16_000_000, transcendentals=0)


def shift(x, hops):
    count = lax.axis_size("col")
    return lax.ppermute(x, "col", [(c, (c + 2 * hops) % count) for c in range(count)])


def sibling(x):
    count = lax.axis_size("col")
    return lax.ppermute(x, "col", [(c, c ^ 1) for c in range(count)])


def ring_first(x):
    return shift(x, 1), shift(x, -1), sibling(x)


def ring_rest(x, first):
    z_count = lax.axis_size("col") // 2
    left, right, near = first
    mine, other = [x] + [None] * (z_count - 1), [near] + [None] * (z_count - 1)
    middle = z_count // 2
    from_left, from_right = x, x
    for hop in range(1, middle):
        from_left = left if hop == 1 else shift(from_left, 1)
        from_right = right if hop == 1 else shift(from_right, -1)
        mine[z_count - hop], mine[hop] = from_left, from_right
        other[z_count - hop], other[hop] = sibling(from_left), sibling(from_right)
    half = x.shape[0] // 2
    top, bottom = shift(from_left[:half], 1), shift(from_right[half:], -1)
    mine[middle] = jnp.concatenate([top, bottom], axis=0)
    other[middle] = jnp.concatenate([sibling(top), sibling(bottom)], axis=0)
    return mine, other


def across_rows(x):
    count = lax.axis_size("row")
    return [x] + [
        lax.ppermute(x, "row", [(r, r ^ d) for r in range(count)]) for d in range(1, count)
    ]


def on_device(factors):
    members = factors.shape[0]
    return jnp.stack([one_factor(factors[m]) for m in range(members)])


def one_factor(factor):
    rows_dev, cols_dev = factor.shape
    col_count, row_count = lax.axis_size("col"), lax.axis_size("row")
    z_count = col_count // 2
    order = rows_dev * row_count
    row_id, col_id = lax.axis_index("row"), lax.axis_index("col")
    z_id, core = col_id // 2, col_id % 2
    bpr = rows_dev // cols_dev
    slab = P_SIZE // col_count
    width = STEPS * slab
    total = STEPS * P_SIZE
    blocks = total // TILE
    row_global = row_id * rows_dev + jnp.arange(rows_dev, dtype=jnp.int32)
    col_global = col_id * cols_dev + jnp.arange(cols_dev, dtype=jnp.int32)
    on_diagonal = row_global[:, None] == col_global[None, :]
    local_trace = jnp.sum(jnp.where(on_diagonal, factor, 0.0))

    cols = factor[:, :width]
    rows = factor.reshape(bpr, cols_dev, cols_dev)[:, :width, :]
    diag = rows[:, :, :width].reshape(bpr * width, width)
    piece = jnp.concatenate([diag, jnp.full((8, width), local_trace)], axis=0)
    slabs = jnp.stack(across_rows(piece))
    mine, other = ring_rest(slabs, ring_first(slabs))
    gathered = jnp.stack([jnp.stack(mine), jnp.stack(other)])
    gathered, cols, rows = lax.optimization_barrier((gathered, cols, rows))

    first = ring_first(cols)
    row_pieces = across_rows(rows.reshape(bpr * width, cols_dev))
    at = jnp.stack([row_id, z_id, core]).astype(jnp.int32)
    square = jax.ShapeDtypeStruct((total, total), jnp.float32)
    params = pltpu.CompilerParams(vmem_limit_bytes=40 * 1024 * 1024)
    part, low = pl.pallas_call(
        functools.partial(place_kernel, 0, blocks // 2, bpr, slab, order),
        out_shape=(square, square),
        in_specs=[in_smem] + in_vmem(1),
        out_specs=tuple(in_vmem(2)),
        compiler_params=params,
        cost_estimate=cost(30_000_000_000),
    )(at, gathered)
    part, low, first = lax.optimization_barrier((part, low, first))
    mine, other = ring_rest(cols, first)
    inv, own = pl.pallas_call(
        functools.partial(finish_kernel, blocks // 2, blocks, bpr, slab, col_count),
        out_shape=(
            jax.ShapeDtypeStruct((col_count, total, width), jnp.float32),
            jax.ShapeDtypeStruct((bpr, width, width), jnp.float32),
        ),
        in_specs=[in_smem] + in_vmem(2),
        out_specs=tuple(in_vmem(2)),
        scratch_shapes=[pltpu.VMEM((total, total), jnp.float32)] * 2,
        compiler_params=params,
        cost_estimate=cost(25_000_000_000),
    )(at, part, low)
    damping = damping_share * jnp.sum(gathered[:, :, :, bpr * width, 0]) / order

    inv_rows = [
        lax.dynamic_index_in_dim(inv, (row_id ^ d) * bpr + b, 0, keepdims=False)
        for d in range(row_count)
        for b in range(bpr)
    ]
    inv_cols = [
        lax.dynamic_index_in_dim(
            inv, (z_id + z) % z_count * 2 + (core ^ side), 0, keepdims=False
        )
        for side in range(2)
        for z in range(z_count)
    ]
    cross = dot(
        jnp.concatenate(inv_rows, axis=1), jnp.concatenate(row_pieces, axis=0), ((1,), (0,))
    )
    lower = dot(
        jnp.concatenate(mine + other, axis=1), jnp.concatenate(inv_cols, axis=1), ((1,), (1,))
    )
    update = dot(lower, cross, ((1,), (0,)), three_pass)

    lower5 = lower.reshape(rows_dev, STEPS, col_count, slab)
    new_cols = lax.dynamic_index_in_dim(lower5, col_id, 2, keepdims=False)
    new_cols = new_cols.reshape(bpr, cols_dev, width)
    new_cols = new_cols.at[:, :width, :].set(own).reshape(rows_dev, width)

    trailing = (row_global % cols_dev >= width)[:, None] & (col_global % cols_dev >= width)[None, :]
    working = factor + jnp.where(on_diagonal, damping, 0.0)
    out = jnp.where(trailing, working - update, 0.0)
    return out.at[:, :width].set(new_cols)


def solution(mesh):
    placed = (P(None, "row", "col"),)
    return jax.shard_map(
        on_device, mesh=mesh, in_specs=placed, out_specs=P(None, "row", "col"), check_vma=False
    )
```
